32 devices in a mesh: expert: 4 (over y, x), dp: 2 (over core), mp: 4 (over z).
Axes of the slice: x: 2, y: 2, z: 4, core: 2. Of those that a mesh axis runs over, the one named last changes fastest.
Arguments:
- tokens: bfloat16 [96, 4096], P(('expert', 'dp'), 'mp'), may hold values from -6 to 6
- routes: int32 [96, 2], P(('expert', 'dp')), may hold values from 0 to 3, all different within a row; in each aligned block of 12 rows (0 to 11, 12 to 23, ...) at most 9 rows name the same one
- router_weight: bfloat16 [4096, 4], P('mp'), may hold values from -0.09375 to 0.09375
- gate_weight: bfloat16 [4, 4096, 16384], P('expert', None, ('dp', 'mp')), may hold values from -0.09375 to 0.09375
- up_weight: bfloat16 [4, 4096, 16384], P('expert', None, ('dp', 'mp')), may hold values from -0.09375 to 0.09375
- down_weight: bfloat16 [4, 16384, 4096], P('expert', ('dp', 'mp')), may hold values from -0.0625 to 0.0625
Outputs:
- mixed: bfloat16 [96, 4096], P(('expert', 'dp'), 'mp')
The draws below stay inside these ranges and needn't reach their ends.
Inputs may be any that keep to these rules, and one draw needn't show every extreme that they name: `routes`: each row names two different experts; among the 12 rows of one device (aligned blocks) no expert is named more than 9 times, a bound that some block reaches.
All inputs are finite; a program needn't handle non-finite values.
Results may differ from the reference program's by a relative error of at most 0.0049.
Values may be sent and summed in bfloat16 or wider, within the bound.
No kernel may reach another device: no remote copies, remote signals or barrier semaphores. Data moves between devices by JAX's collectives and lax.ppermute only.
A program may use at most 128 MiB of HBM per device.

```python
import math
import jax
import jax.numpy as jnp
import numpy as np
from jax import lax

D = 4096
FF = 16384
TOP = 2
TOK_DEV = 12
EXPERTS = 4
CAP = 9
TOKENS = 96


def with_spikes(entries, stream_key, source, target, shards_of, factor):
    owner, partner = [(jnp.arange(entries.shape[dim]) // (entries.shape[dim] // shards_of)).reshape([-1 if axis == dim else 1 for axis in range(entries.ndim)]) for dim in (source, target)]
    chosen = jax.random.permutation(stream_key, shards_of)[partner]
    strong = (owner == chosen) | (owner == (partner + shards_of // 2) % shards_of)
    return jnp.where(strong, factor * entries, entries)


def block_scale(key, shape, split, smallest, high):
    loudness, own = 1.0, jax.random.fold_in(key, 6)
    for dim, blocks in split:
        steps = jnp.exp(jax.random.uniform(jax.random.fold_in(own, dim), (blocks,), jnp.float32, smallest / len(split), high / len(split)))
        loudness = loudness * jnp.repeat(steps, shape[dim] // blocks).reshape([-1 if axis == dim else 1 for axis in range(len(shape))])
    return loudness


def shared_out(own_key, own, number, rows, amount, top, most, lean):
    ranking = jax.random.permutation(own_key, amount)
    crowded, usual = portions_of(amount, rows * top, most, lean, True), portions_of(amount, rows * top, most, lean, False)
    places = jnp.arange(amount)

    def named(lengths, rotation):
        used = int((lengths > 0).sum())
        fixed = max(1, used // 4)
        shifted = fixed + (places - fixed + rotation * (used - fixed)) % max(1, amount - fixed)
        return jnp.zeros((amount,), jnp.int32).at[ranking[jnp.where(places < fixed, places, shifted)]].set(jnp.asarray(lengths, jnp.int32))

    lengths = jnp.where(number % 4 == 0, named(crowded, number // 4), named(usual, number - number // 4 - 1))
    mixed = jax.random.permutation(jax.random.fold_in(own, 3), amount)
    source_of, taker = mixed[0:amount // 2 * 2:2], mixed[1:amount // 2 * 2:2]
    margin = jnp.minimum(lengths[source_of] - 1, most - lengths[taker]) // 2
    margin = jnp.where((source_of == ranking[0]) | (taker == ranking[0]) | (lengths[taker] == 0), 0, jnp.maximum(margin, 0))
    shifted = jax.random.randint(jax.random.fold_in(own, 4), (amount // 2,), 0, 1 << 20) % (margin + 1)
    lengths = lengths.at[source_of].add(-shifted).at[taker].add(shifted)
    items = jnp.searchsorted(jnp.cumsum(lengths), jnp.arange(rows * top), side="right").astype(jnp.int32)
    listing = items.reshape(top, rows).T
    listing = listing[jax.random.permutation(jax.random.fold_in(own, 1), rows)]
    rotation = jax.random.randint(jax.random.fold_in(own, 2), (rows, 1), 0, top)
    return jnp.take_along_axis(listing, (jnp.arange(top)[None, :] + rotation) % top, axis=1)


def portions_of(amount, total, most, lean, full):
    loads = [(1 << 20) // math.isqrt(grade ** lean) + 1 for grade in range(1, amount + 1)]
    largest = most if full else min(most, max(-(-total // amount), total * loads[0] // sum(loads)))
    least = 1 if total - largest >= amount - 1 else 0
    holding, surplus = [largest] + [least] * (amount - 1), total - largest - least * (amount - 1)
    while surplus > 0:
        free = [i for i in range(1, amount) if holding[i] < largest] or [i for i in range(1, amount) if holding[i] < most]
        mass, remaining = sum([loads[i] for i in free]), surplus
        for i in free:
            addition = min(most - holding[i], max(1, remaining * loads[i] // mass), surplus)
            holding[i] = holding[i] + addition
            surplus = surplus - addition
    return np.array(holding)


def bell_draw(rng, shape, width, limit, pieces=(), held_as=jnp.bfloat16):
    values = jax.random.normal(rng, shape, jnp.float32) * width
    if len(pieces) > 0:
        values = block_scale(rng, shape, pieces, -0.22, 0.18) * values
    return jnp.clip(values, min=-limit, max=limit).astype(held_as)


def noise_with(own_key, dims, spread, bound, split, heavy, kind=jnp.bfloat16):
    entries = spread * jax.random.normal(own_key, dims, jnp.float32)
    if split:
        entries = entries * block_scale(own_key, dims, split, -0.22, 0.18)
    return jnp.clip(with_spikes(entries, jax.random.fold_in(own_key, 3), *heavy), -bound, bound).astype(kind)


def setup_inputs(seed: int = 0) -> dict:
    keys = jax.random.split(jax.random.key(seed), 7)
    tokens = bell_draw(keys[0], (TOKENS, D), 1.0, 6.0, ((0, 8), (1, 4)))
    routes_keys = jax.random.split(jax.random.fold_in(keys[1], 1), TOKENS // TOK_DEV)
    routes_turns = jax.random.permutation(jax.random.fold_in(keys[1], 3), TOKENS // TOK_DEV)
    routes = jax.vmap(lambda own, number: shared_out(jax.random.fold_in(keys[1], 2), own, number, TOK_DEV, EXPERTS, TOP, CAP, 2))(routes_keys, routes_turns).reshape((TOKENS, TOP))
    router_weight = bell_draw(keys[2], (D, EXPERTS), D ** -0.5, 0.09375, ((0, 4),))
    gate_weight = bell_draw(keys[3], (EXPERTS, D, FF), D ** -0.5, 0.09375, ((0, 4), (2, 8)))
    up_weight = bell_draw(keys[4], (EXPERTS, D, FF), D ** -0.5, 0.09375, ((0, 4), (2, 8)))
    down_weight = noise_with(keys[5], (EXPERTS, FF, D), FF ** -0.5, 0.0625, ((0, 4), (1, 8)), (1, 2, 8, 2.0))
    return {"tokens": tokens, "routes": routes, "router_weight": router_weight, "gate_weight": gate_weight, "up_weight": up_weight, "down_weight": down_weight}


def reference(tokens, routes, router_weight, gate_weight, up_weight, down_weight):
    blocks = TOKENS // TOK_DEV
    logits = jnp.dot(tokens, router_weight, preferred_element_type=jnp.float32)
    labels = jnp.arange(EXPERTS, dtype=jnp.int32)
    onehot = (routes[:, :, None] == labels).astype(jnp.int32)
    chosen = jnp.sum(onehot.astype(jnp.float32) * logits[:, None, :], axis=2)
    weights = jnp.stack([jax.nn.sigmoid(chosen[:, 0] - chosen[:, 1]), jax.nn.sigmoid(chosen[:, 1] - chosen[:, 0])], axis=1)
    flat_hot = onehot.reshape(blocks, TOK_DEV * TOP, EXPERTS)
    before = jnp.cumsum(flat_hot, axis=1) - flat_hot
    position = jnp.sum(flat_hot * before, axis=2)
    places = (position[:, :, None] == jnp.arange(CAP, dtype=jnp.int32)).astype(jnp.float32)
    assign = flat_hot.astype(jnp.float32)[:, :, :, None] * places[:, :, None, :]
    assign = assign.reshape(blocks, TOK_DEV, TOP, EXPERTS, CAP)
    select = jnp.sum(assign, axis=2)
    combine = jnp.sum(assign * weights.reshape(blocks, TOK_DEV, TOP)[:, :, :, None, None], axis=2)
    grouped = tokens.reshape(blocks, TOK_DEV, D).astype(jnp.float32)
    buffers = jnp.einsum("btec,btd->ebcd", select, grouped, precision=lax.Precision.HIGHEST).astype(jnp.bfloat16)

    def expert(packed):
        inputs, w_gate, w_up, w_down = packed
        inputs = inputs.reshape(blocks * CAP, D)
        gate_part = jnp.dot(inputs, w_gate, preferred_element_type=jnp.float32)
        up_part = jnp.dot(inputs, w_up, preferred_element_type=jnp.float32)
        hidden = (jax.nn.silu(gate_part) * up_part).astype(jnp.bfloat16)
        return jnp.dot(hidden, w_down, preferred_element_type=jnp.float32).reshape(blocks, CAP, D)

    outputs = lax.map(expert, (buffers, gate_weight, up_weight, down_weight))
    mixed_out = jnp.einsum("btec,ebcd->btd", combine, outputs, precision=lax.Precision.HIGHEST)
    return mixed_out.reshape(TOKENS, D).astype(jnp.bfloat16)
```

```python
import functools

import jax
import jax.numpy as jnp
from jax import lax
from jax.experimental import pallas as pl
from jax.experimental.pallas import tpu as pltpu
from jax.sharding import PartitionSpec as P


VMEM = pl.BlockSpec(memory_space=pltpu.VMEM)
MIB = 1 << 20
HINT = 3 * 10**10


def call(body, out_shape, args, scratch=(), limit=2 * MIB, flops=0, moved=0):
    single = not isinstance(out_shape, (tuple, list))
    return pl.pallas_call(
        body,
        out_shape=out_shape,
        in_specs=[VMEM] * len(args),
        out_specs=VMEM if single else [VMEM] * len(out_shape),
        scratch_shapes=list(scratch),
        compiler_params=pltpu.CompilerParams(vmem_limit_bytes=limit),
        cost_estimate=pl.CostEstimate(flops=flops, bytes_accessed=moved, transcendentals=0),
    )(*[pltpu.with_memory_space_constraint(a, pltpu.VMEM) for a in args])


def shape(dims, dtype):
    return pltpu.VMEM(tuple(dims), dtype)


def swap(value, axis, size, shift):
    return lax.ppermute(value, axis, [(i, i ^ shift) for i in range(size)])


def send(value, axis, size, shift):
    return lax.ppermute(value, axis, [(i, (i + shift) % size) for i in range(size)])


def stack(value):
    half = value.shape[1] // 2
    return jnp.concatenate([value[:, :half], value[:, half:]], axis=0)


def unstack(value):
    half = value.shape[0] // 2
    return jnp.concatenate([value[:half], value[half:]], axis=1)


def pack_kernel(tokens, router, out):
    out[...] = jnp.concatenate(
        [tokens[...].astype(jnp.float32), router[...].astype(jnp.float32)], axis=0
    ).astype(out.dtype)


def join_kernel(rows, *refs):
    *blocks, out = refs
    wide = jnp.concatenate([b[:rows, :].astype(jnp.float32) for b in blocks], axis=1)
    out[...] = stack(wide).astype(out.dtype)


def weigh_kernel(rows, experts, routes, *refs):
    *blocks, out = refs
    logits = None
    for b in blocks:
        term = lax.dot_general(
            b[:rows, :],
            b[rows:, :],
            (((1,), (1,)), ((), ())),
            preferred_element_type=jnp.float32,
        )
        logits = term if logits is None else logits + term
    label = lax.broadcasted_iota(jnp.int32, (rows, experts), 1)
    first, second = routes[:, 0:1], routes[:, 1:2]
    chosen_first = jnp.sum(jnp.where(label == first, logits, 0.0), axis=1, keepdims=True)
    chosen_second = jnp.sum(jnp.where(label == second, logits, 0.0), axis=1, keepdims=True)
    weight_first = jax.nn.sigmoid(chosen_first - chosen_second)
    weight_second = jax.nn.sigmoid(chosen_second - chosen_first)
    mine = lax.bitwise_xor(label, lax.axis_index("expert"))
    out[...] = jnp.where(
        mine == first, weight_first, jnp.where(mine == second, weight_second, 0.0)
    )


def hidden_kernel(rows, pad, width_parts, *refs):
    *sources, gate, up, h, x = refs
    filler = jnp.zeros((pad - rows, x.shape[1]), jnp.float32)
    for i, source in enumerate(sources):
        wide = unstack(source[...].astype(jnp.float32))
        x[pad * i : pad * (i + 1), :] = jnp.concatenate([wide, filler], axis=0).astype(x.dtype)
    part = x.shape[1] // width_parts
    block = 256 if h.shape[1] % 256 == 0 else h.shape[1]

    def step(n, carry):
        columns = pl.ds(pl.multiple_of(n * block, block), block)
        sums = []
        for weight in (gate, up):
            total = None
            for s in range(width_parts):
                where = lax.rem(lax.axis_index("mp") - s + width_parts, width_parts)
                slab = weight[pl.ds(pl.multiple_of(where * part, part), part), columns]
                term = jnp.dot(
                    x[:, part * s : part * (s + 1)], slab, preferred_element_type=jnp.float32
                )
                total = term if total is None else total + term
            sums.append(total)
        g, u = sums
        h[:, columns] = (g / (1.0 + jnp.exp(-g)) * u).astype(h.dtype)
        return carry

    lax.fori_loop(0, h.shape[1] // block, step, 0)


def down_kernel(h, down, sent, kept):
    half = kept.shape[0]
    wide = 512 if down.shape[1] % 512 == 0 else down.shape[1]

    def step(n, carry):
        columns = pl.ds(pl.multiple_of(n * wide, wide), wide)
        result = jnp.dot(h[...], down[:, columns], preferred_element_type=jnp.float32)
        kept[:, columns] = result[:half]
        sent[:, columns] = result[half:].astype(sent.dtype)
        return carry

    lax.fori_loop(0, down.shape[1] // wide, step, 0)


def pair_kernel(rows, pad, kept, got, *outs):
    for i, out in enumerate(outs):
        total = kept[pad * i : pad * i + rows, :] + got[pad * i : pad * i + rows, :].astype(jnp.float32)
        out[...] = total if i == 0 else stack(total).astype(out.dtype)


def mix_kernel(weights, own, *refs):
    others = refs[: weights.shape[1] - 1]
    *outs, total = refs[weights.shape[1] - 1 :]
    sum_ = own[...] * weights[:, 0:1]
    for s, got in enumerate(others, 1):
        sum_ = sum_ + unstack(got[...].astype(jnp.float32)) * weights[:, s : s + 1]
    total[...] = sum_
    parts = len(outs)
    part = total.shape[1] // parts
    for s, out in enumerate(outs):
        where = lax.rem(lax.axis_index("mp") + s, parts)
        piece = total[:, pl.ds(pl.multiple_of(where * part, part), part)]
        out[...] = piece if s == 0 else stack(piece).astype(out.dtype)


def final_kernel(own, *refs):
    *others, out = refs
    total = own[...]
    for got in others:
        total = total + unstack(got[...].astype(jnp.float32))
    out[...] = total.astype(out.dtype)


def fast(tokens, routes, router_weight, gate_weight, up_weight, down_weight):
    experts, dp, mp = (lax.axis_size(a) for a in ("expert", "dp", "mp"))
    rows, part = tokens.shape
    hidden = gate_weight.shape[2]
    width = part * mp
    pad = -(-rows // 16) * 16
    bf16, f32 = jnp.bfloat16, jnp.float32
    packed = call(pack_kernel, shape((rows + experts, part), bf16), [tokens, router_weight.T])
    blocks = [packed] + [send(packed, "mp", mp, s) for s in range(1, mp)]
    joined = call(functools.partial(join_kernel, rows), shape((2 * rows, width // 2), bf16), blocks, flops=HINT)
    near = [joined] + [swap(joined, "expert", experts, s) for s in range(1, experts)]
    weights = call(
        functools.partial(weigh_kernel, rows, experts), shape((rows, experts), f32), [routes] + blocks
    )
    far = [swap(value, "dp", dp, 1) for value in near]
    count = len(near)
    total_rows = 2 * count * pad
    h = call(
        functools.partial(hidden_kernel, rows, pad, mp),
        shape((total_rows, hidden), bf16),
        near + far + [gate_weight[0], up_weight[0]],
        scratch=[pltpu.VMEM((total_rows, width), bf16)],
        limit=8 * MIB,
        flops=4 * total_rows * width * hidden,
        moved=4 * width * hidden,
    )
    sent, kept = call(
        down_kernel,
        [shape((count * pad, width), bf16), shape((count * pad, width), f32)],
        [h, down_weight[0]],
        limit=6 * MIB,
        flops=2 * total_rows * width * hidden,
        moved=2 * width * hidden,
    )
    got = swap(sent, "dp", dp, 1)
    totals = call(
        functools.partial(pair_kernel, rows, pad),
        [shape((rows, width), f32)] + [shape((2 * rows, width // 2), bf16)] * (count - 1),
        [kept, got],
        limit=4 * MIB,
    )
    back = [swap(totals[s], "expert", experts, s) for s in range(1, count)]
    pieces = call(
        mix_kernel,
        [shape((rows, part), f32)] + [shape((2 * rows, part // 2), bf16)] * (mp - 1),
        [weights, totals[0]] + back,
        scratch=[pltpu.VMEM((rows, width), f32)],
    )
    last = [send(pieces[s], "mp", mp, s) for s in range(1, mp)]
    return call(final_kernel, jax.ShapeDtypeStruct((rows, part), bf16), [pieces[0]] + last)


def per_device(tokens, routes, router_weight, gate_weight, up_weight, down_weight):
    experts, dp = lax.axis_size("expert"), lax.axis_size("dp")
    small = dp == 2 and experts & (experts - 1) == 0 and experts * dp * tokens.shape[0] <= 256
    body = fast if small else plain
    return body(tokens, routes, router_weight, gate_weight, up_weight, down_weight)


def plain(tokens, routes, router_weight, gate_weight, up_weight, down_weight):
    row_count = tokens.shape[0]
    experts = lax.axis_size("expert")
    capacity = max(2, (6 * row_count + 2 * experts - 1) // (2 * experts))
    partial_logits = jnp.dot(tokens, router_weight, preferred_element_type=jnp.float32)
    logits = lax.psum(partial_logits, "mp")
    labels = jnp.arange(experts, dtype=jnp.int32)
    onehot = (routes[:, :, None] == labels).astype(jnp.int32)
    chosen = jnp.sum(onehot.astype(jnp.float32) * logits[:, None, :], axis=2)
    weights = jnp.stack(
        [jax.nn.sigmoid(chosen[:, 0] - chosen[:, 1]), jax.nn.sigmoid(chosen[:, 1] - chosen[:, 0])],
        axis=1,
    )
    flat_hot = onehot.reshape(row_count * 2, experts)
    before = jnp.cumsum(flat_hot, axis=0) - flat_hot
    position = jnp.sum(flat_hot * before, axis=1)
    places = (position[:, None] == jnp.arange(capacity, dtype=jnp.int32)).astype(jnp.float32)
    assign = (flat_hot.astype(jnp.float32)[:, :, None] * places[:, None, :]).reshape(
        row_count, 2, experts, capacity
    )
    select = jnp.sum(assign, axis=1).astype(jnp.bfloat16)
    combine = jnp.sum(assign * weights[:, :, None, None], axis=1).reshape(
        row_count, experts * capacity
    )
    full_rows = lax.all_gather(tokens, "mp", axis=1, tiled=True)
    full_width = full_rows.shape[1]
    buffer = jnp.einsum(
        "tec,td->ecd", select, full_rows, preferred_element_type=jnp.float32
    ).astype(jnp.bfloat16)
    arrived = lax.all_to_all(buffer, "expert", split_axis=0, concat_axis=0, tiled=True)
    inputs = lax.all_gather(
        arrived.reshape(experts * capacity, full_width), "dp", axis=0, tiled=True
    )
    gate_part = jnp.dot(inputs, gate_weight[0], preferred_element_type=jnp.float32)
    up_part = jnp.dot(inputs, up_weight[0], preferred_element_type=jnp.float32)
    hidden = (jax.nn.silu(gate_part) * up_part).astype(jnp.bfloat16)
    summed = lax.psum_scatter(
        jnp.dot(hidden, down_weight[0], preferred_element_type=jnp.float32),
        "dp",
        scatter_dimension=0,
        tiled=True,
    )
    returned = lax.all_to_all(
        summed.reshape(experts, capacity, full_width),
        "expert",
        split_axis=0,
        concat_axis=0,
        tiled=True,
    )
    partial_mix = jnp.dot(
        combine,
        returned.reshape(experts * capacity, full_width),
        precision=lax.Precision.HIGHEST,
        preferred_element_type=jnp.float32,
    )
    mixed_out = lax.psum_scatter(partial_mix, "mp", scatter_dimension=1, tiled=True)
    return mixed_out.astype(jnp.bfloat16)


def solution(mesh):
    return jax.shard_map(
        per_device,
        mesh=mesh,
        in_specs=(
            P(("expert", "dp"), "mp"),
            P(("expert", "dp"), None),
            P("mp", None),
            P("expert", None, ("dp", "mp")),
            P("expert", None, ("dp", "mp")),
            P("expert", ("dp", "mp"), None),
        ),
        out_specs=P(("expert", "dp"), "mp"),
        check_vma=False,
    )
```

```python
import functools

import jax
import jax.numpy as jnp
from jax import lax
from jax.experimental import pallas as pl
from jax.experimental.pallas import tpu as pltpu
from jax.sharding import PartitionSpec as P


VMEM = pl.BlockSpec(memory_space=pltpu.VMEM)
MIB = 1 << 20
HINT = 3 * 10**10
HIDDEN_HINT = 10**8


def call(body, out_shape, args, scratch=(), limit=2 * MIB, flops=0, moved=0, space=pltpu.VMEM):
    single = not isinstance(out_shape, (tuple, list))
    return pl.pallas_call(
        body,
        out_shape=out_shape,
        in_specs=[pl.BlockSpec(memory_space=space)] * len(args),
        out_specs=VMEM if single else [VMEM] * len(out_shape),
        scratch_shapes=list(scratch),
        compiler_params=pltpu.CompilerParams(vmem_limit_bytes=limit),
        cost_estimate=pl.CostEstimate(flops=flops, bytes_accessed=moved, transcendentals=0),
    )(*[pltpu.with_memory_space_constraint(a, space) for a in args])


def shape(dims, dtype):
    return pltpu.VMEM(tuple(dims), dtype)


def swap(value, axis, size, shift):
    return lax.ppermute(value, axis, [(i, i ^ shift) for i in range(size)])


def send(value, axis, size, shift):
    return lax.ppermute(value, axis, [(i, (i + shift) % size) for i in range(size)])


def stack(value):
    half = value.shape[1] // 2
    return jnp.concatenate([value[:, :half], value[:, half:]], axis=0)


def unstack(value):
    half = value.shape[0] // 2
    return jnp.concatenate([value[:half], value[half:]], axis=1)


def pack_kernel(tokens, router, out, held_tokens, held_router, sem):
    copies = [
        pltpu.make_async_copy(tokens, held_tokens, sem.at[0]),
        pltpu.make_async_copy(router, held_router, sem.at[1]),
    ]
    for copy in copies:
        copy.start()
    for copy in copies:
        copy.wait()
    out[...] = jnp.concatenate(
        [held_tokens[...].astype(jnp.float32), held_router[...].astype(jnp.float32)], axis=0
    ).astype(out.dtype)


def join_kernel(rows, *refs):
    *blocks, out = refs
    wide = jnp.concatenate([b[:rows, :].astype(jnp.float32) for b in blocks], axis=1)
    out[...] = stack(wide).astype(out.dtype)


def weigh_kernel(rows, experts, routes, *refs):
    *blocks, out = refs
    logits = None
    for b in blocks:
        term = lax.dot_general(
            b[:rows, :],
            b[rows:, :],
            (((1,), (1,)), ((), ())),
            preferred_element_type=jnp.float32,
        )
        logits = term if logits is None else logits + term
    label = lax.broadcasted_iota(jnp.int32, (rows, experts), 1)
    first, second = routes[:, 0:1], routes[:, 1:2]
    chosen_first = jnp.sum(jnp.where(label == first, logits, 0.0), axis=1, keepdims=True)
    chosen_second = jnp.sum(jnp.where(label == second, logits, 0.0), axis=1, keepdims=True)
    weight_first = jax.nn.sigmoid(chosen_first - chosen_second)
    weight_second = jax.nn.sigmoid(chosen_second - chosen_first)
    mine = lax.bitwise_xor(label, lax.axis_index("expert"))
    out[...] = jnp.where(
        mine == first, weight_first, jnp.where(mine == second, weight_second, 0.0)
    )


def hidden_kernel(rows, pad, width_parts, *refs):
    *sources, gate, up, _, h, x = refs
    part = x.shape[1] // width_parts
    filler = jnp.zeros((pad - rows, part), jnp.float32)
    for i, source in enumerate(sources):
        wide = unstack(source[...].astype(jnp.float32))
        for s in range(width_parts):
            where = lax.rem(lax.axis_index("mp") - s + width_parts, width_parts)
            columns = pl.ds(pl.multiple_of(where * part, part), part)
            piece = wide[:, part * s : part * (s + 1)]
            x[pad * i : pad * (i + 1), columns] = jnp.concatenate([piece, filler], axis=0).astype(x.dtype)
    block = h.shape[1]

    def step(n, carry):
        columns = pl.ds(pl.multiple_of(n * block, block), block)
        sums = []
        for weight in (gate, up):
            total = jnp.dot(x[...], weight[:, columns], preferred_element_type=jnp.float32)
            sums.append(total)
        g, u = sums
        h[:, columns] = (g / (1.0 + jnp.exp(-g)) * u).astype(h.dtype)
        return carry

    lax.fori_loop(0, h.shape[1] // block, step, 0)


def held_slices(core):
    return 2 * core, 3 - 2 * core


def down_kernel(rows, pad, other, h, down, out):
    core = lax.axis_index("dp")
    owner = 1 - core if other else core
    half = out.shape[1] // 2
    count = h.shape[0] // (2 * pad)
    for i, offset in enumerate(held_slices(owner)):
        where = lax.bitwise_xor(lax.axis_index("mp"), offset)
        columns = pl.ds(pl.multiple_of(where * half, half), half)
        result = jnp.dot(h[...], down[:, columns], preferred_element_type=jnp.float32)
        pieces = []
        for s in range(count):
            pair = [result[pad * k : pad * k + rows] for k in (s, count + s)]
            pieces += pair[::-1] if other else pair
        out[:, half * i : half * (i + 1)] = jnp.concatenate(pieces, axis=0).astype(out.dtype)


def pair_kernel(kept, got, *outs):
    deep = kept.shape[0] // len(outs)
    for i, out in enumerate(outs):
        block = pl.ds(deep * i, deep)
        out[...] = (kept[block, :] + got[block, :].astype(jnp.float32)).astype(out.dtype)


def mix_kernel(weights, weights_other, own, *refs):
    *others, kept, far, near = refs
    factor = jnp.concatenate([weights[...], weights_other[...]], axis=0)
    total = own[...] * factor[:, 0:1]
    for s, got in enumerate(others, 1):
        total = total + got[...].astype(jnp.float32) * factor[:, s : s + 1]
    half = total.shape[1] // 2
    left, right = total[:, :half], total[:, half:]
    first = lax.axis_index("dp") == 0
    kept[...] = jnp.where(first, left, 0.0)
    far[...] = jnp.where(first, right, left).astype(far.dtype)
    near[...] = right.astype(near.dtype)


def slice_kernel(kept, far, near, own, other):
    last = jnp.where(lax.axis_index("dp") == 1, near[...].astype(jnp.float32), 0.0)
    total = kept[...] + far[...].astype(jnp.float32) + last
    rows = own.shape[0]
    own[...] = total[:rows]
    other[...] = total[rows:]


def final_kernel(own, got, out):
    out[...] = (own[...] + got[...]).astype(out.dtype)


def cores_apart(value, first, second):
    size = lax.axis_size("mp")
    pairs = [
        (core * size + i, core * size + (i ^ step))
        for core, step in enumerate((first, second))
        for i in range(size)
        if step
    ]
    return lax.ppermute(value, ("dp", "mp"), pairs)


def fast(tokens, routes, router_weight, gate_weight, up_weight, down_weight):
    experts, dp, mp = (lax.axis_size(a) for a in ("expert", "dp", "mp"))
    rows, part = tokens.shape
    hidden = gate_weight.shape[2]
    width = part * mp
    pad = -(-rows // 16) * 16
    bf16, f32 = jnp.bfloat16, jnp.float32
    packed = call(
        pack_kernel,
        shape((rows + experts, part), bf16),
        [tokens, router_weight.T],
        scratch=[
            pltpu.VMEM((rows, part), bf16),
            pltpu.VMEM((experts, part), bf16),
            pltpu.SemaphoreType.DMA((2,)),
        ],
        space=pltpu.HBM,
    )
    blocks = [packed]
    for s in range(1, mp):
        blocks.append(send(packed, "mp", mp, s))
    joined = call(
        functools.partial(join_kernel, rows),
        shape((2 * rows, width // 2), bf16),
        blocks,
        flops=HINT,
    )
    near = [joined]
    for s in range(1, experts):
        near.append(swap(joined, "expert", experts, s))
    weights = call(
        functools.partial(weigh_kernel, rows, experts), shape((rows, experts), f32), [routes] + blocks
    )
    weights_other = swap(weights, "dp", dp, 1)
    far = [swap(value, "dp", dp, 1) for value in near]
    total_rows = 2 * experts * pad
    h = call(
        functools.partial(hidden_kernel, rows, pad, mp),
        shape((total_rows, hidden), bf16),
        near + far + [gate_weight[0], up_weight[0], down_weight[0]],
        scratch=[pltpu.VMEM((total_rows, width), bf16)],
        limit=8 * MIB,
        flops=HIDDEN_HINT,
        moved=4 * width * hidden,
    )
    partial = {}
    for other in (True, False):
        partial[other] = call(
            functools.partial(down_kernel, rows, pad, other),
            shape((2 * experts * rows, width // 2), bf16 if other else f32),
            [h, down_weight[0]],
            limit=6 * MIB,
            flops=total_rows * width * hidden,
            moved=width * hidden,
        )
    got = swap(partial[True], "dp", dp, 1)
    deep = 2 * rows
    totals = call(
        pair_kernel,
        [shape((deep, width // 2), f32)] + [shape((deep, width // 2), bf16)] * (experts - 1),
        [partial[False], got],
        limit=4 * MIB,
    )
    back = []
    for s in range(1, experts):
        back.append(swap(totals[s], "expert", experts, s))
    kept, far_slice, near_slice = call(
        mix_kernel,
        [shape((deep, part), f32), shape((deep, part), bf16), shape((deep, part), bf16)],
        [weights, weights_other, totals[0]] + back,
        limit=4 * MIB,
    )
    near_slice = cores_apart(near_slice, 1, 1)
    far_slice = cores_apart(far_slice, 3, 2)
    own, other = call(
        slice_kernel, [shape((rows, part), f32)] * 2, [kept, far_slice, near_slice]
    )
    return call(final_kernel, jax.ShapeDtypeStruct((rows, part), bf16), [own, swap(other, "dp", dp, 1)])


def per_device(tokens, routes, router_weight, gate_weight, up_weight, down_weight):
    square = lax.axis_size("expert") == 4 and lax.axis_size("dp") == 2 and lax.axis_size("mp") == 4
    body = fast if square and tokens.shape[0] <= 16 else plain
    return body(tokens, routes, router_weight, gate_weight, up_weight, down_weight)


def plain(tokens, routes, router_weight, gate_weight, up_weight, down_weight):
    row_count = tokens.shape[0]
    experts = lax.axis_size("expert")
    capacity = max(2, (6 * row_count + 2 * experts - 1) // (2 * experts))
    partial_logits = jnp.dot(tokens, router_weight, preferred_element_type=jnp.float32)
    logits = lax.psum(partial_logits, "mp")
    labels = jnp.arange(experts, dtype=jnp.int32)
    onehot = (routes[:, :, None] == labels).astype(jnp.int32)
    chosen = jnp.sum(onehot.astype(jnp.float32) * logits[:, None, :], axis=2)
    weights = jnp.stack(
        [jax.nn.sigmoid(chosen[:, 0] - chosen[:, 1]), jax.nn.sigmoid(chosen[:, 1] - chosen[:, 0])],
        axis=1,
    )
    flat_hot = onehot.reshape(row_count * 2, experts)
    before = jnp.cumsum(flat_hot, axis=0) - flat_hot
    position = jnp.sum(flat_hot * before, axis=1)
    places = (position[:, None] == jnp.arange(capacity, dtype=jnp.int32)).astype(jnp.float32)
    assign = (flat_hot.astype(jnp.float32)[:, :, None] * places[:, None, :]).reshape(
        row_count, 2, experts, capacity
    )
    select = jnp.sum(assign, axis=1).astype(jnp.bfloat16)
    combine = jnp.sum(assign * weights[:, :, None, None], axis=1).reshape(
        row_count, experts * capacity
    )
    full_rows = lax.all_gather(tokens, "mp", axis=1, tiled=True)
    full_width = full_rows.shape[1]
    buffer = jnp.einsum(
        "tec,td->ecd", select, full_rows, preferred_element_type=jnp.float32
    ).astype(jnp.bfloat16)
    arrived = lax.all_to_all(buffer, "expert", split_axis=0, concat_axis=0, tiled=True)
    inputs = lax.all_gather(
        arrived.reshape(experts * capacity, full_width), "dp", axis=0, tiled=True
    )
    gate_part = jnp.dot(inputs, gate_weight[0], preferred_element_type=jnp.float32)
    up_part = jnp.dot(inputs, up_weight[0], preferred_element_type=jnp.float32)
    hidden = (jax.nn.silu(gate_part) * up_part).astype(jnp.bfloat16)
    summed = lax.psum_scatter(
        jnp.dot(hidden, down_weight[0], preferred_element_type=jnp.float32),
        "dp",
        scatter_dimension=0,
        tiled=True,
    )
    returned = lax.all_to_all(
        summed.reshape(experts, capacity, full_width),
        "expert",
        split_axis=0,
        concat_axis=0,
        tiled=True,
    )
    partial_mix = jnp.dot(
        combine,
        returned.reshape(experts * capacity, full_width),
        precision=lax.Precision.HIGHEST,
        preferred_element_type=jnp.float32,
    )
    mixed_out = lax.psum_scatter(partial_mix, "mp", scatter_dimension=1, tiled=True)
    return mixed_out.astype(jnp.bfloat16)


def solution(mesh):
    return jax.shard_map(
        per_device,
        mesh=mesh,
        in_specs=(
            P(("expert", "dp"), "mp"),
            P(("expert", "dp"), None),
            P("mp", None),
            P("expert", None, ("dp", "mp")),
            P("expert", None, ("dp", "mp")),
            P("expert", ("dp", "mp"), None),
        ),
        out_specs=P(("expert", "dp"), "mp"),
        check_vma=False,
    )
```
